1024 devices in a mesh: dp: 32 (over z, core), expert: 32 (over y, x).
Axes of the slice: x: 4, y: 8, z: 16, core: 2. Of those that a mesh axis runs over, the one named last changes fastest.
Arguments:
- tokens: bfloat16 [262144, 1024], P(('dp', 'expert')), may hold values from -6 to 6
- router: bfloat16 [1024, 32], replicated, may hold values from -0.1875 to 0.1875
- w_in: bfloat16 [32, 1024, 2048], P('expert'), may hold values from -0.1875 to 0.1875
- w_out: bfloat16 [32, 2048, 1024], P('expert'), may hold values from -0.125 to 0.125
- assign: int32 [262144], P(('dp', 'expert')), may hold values from 0 to 31, as said below
- modality: int32 [262144], P(('dp', 'expert')), may hold values from 0 to 1
- slot: int32 [262144], P(('dp', 'expert')), may hold values from 0 to 11, as said below
Outputs:
- mixed: bfloat16 [262144, 1024], P(('dp', 'expert'))
- importance: float32 [2, 32], replicated
- entropies: float32 [2, 2], replicated
The draws below stay inside these ranges and needn't reach their ends.
Inputs may be any that keep to these rules, and one draw needn't show every extreme that they name: `assign`: in the rows of one device each expert is named at most 12 times; in every device's rows one expert is named exactly 12 times, the same expert for all devices of one index of dp. A token's slot is the number of earlier rows of the same device that name the same expert.
All inputs are finite; a program needn't handle non-finite values.
Results may differ from the reference program's by a relative error of at most 0.003.
The reference program's roundings to bfloat16 on the way count: a program that leaves them out, or rounds other values in their place, can miss the bound.
Values may be sent and summed in bfloat16 or wider, within the bound.
No kernel may reach another device: no remote copies, remote signals or barrier semaphores. Data moves between devices by JAX's collectives and lax.ppermute only.
A program may use at most 32 MiB of HBM per device.

```python
import jax
import jax.numpy as jnp
from jax import lax

D = 1024
FF = 2048
TOK_DEV = 256
EXPERTS = 32
CAP = 12
TOKENS = 262144
N_EXPERT = 32
DEVICES = 1024


def joint_routes(key):
    base = jax.random.fold_in(key, 11)
    count = TOKENS // TOK_DEV

    def one_block(index):
        block_key = jax.random.fold_in(base, index)
        row_key = jax.random.fold_in(jax.random.fold_in(base, 100003), index // N_EXPERT)
        filled = jax.random.randint(row_key, (), 0, EXPERTS)
        shuffled = jax.random.permutation(jax.random.fold_in(block_key, 1), EXPERTS * CAP)
        order = jnp.argsort((shuffled // CAP != filled).astype(jnp.int32), stable=True)
        chosen = shuffled[order][:TOK_DEV]
        labels = jax.random.permutation(jax.random.fold_in(block_key, 2), chosen)
        experts_of = (labels // CAP).astype(jnp.int32)
        onehot = (experts_of[:, None] == jnp.arange(EXPERTS, dtype=jnp.int32)[None, :]).astype(jnp.int32)
        before = jnp.cumsum(onehot, axis=0) - onehot
        ranks = jnp.sum(before * onehot, axis=1).astype(jnp.int32)
        return (experts_of, ranks)
    experts_all, ranks_all = jax.vmap(one_block)(jnp.arange(count))
    return (experts_all.reshape(-1).astype(jnp.int32), ranks_all.reshape(-1).astype(jnp.int32))


def draw_assign(key, part):
    return joint_routes(key)[0].astype(jnp.int32)


def draw_slot(key, part):
    return joint_routes(key)[1].astype(jnp.int32)


def with_ends(entries, stream_key, least, largest):
    longest = entries.shape.index(max(entries.shape))
    spots = []
    for shift in (0, 1):
        where = [jax.random.randint(jax.random.fold_in(stream_key, axis), (), 0, length) for axis, length in enumerate(entries.shape)]
        where[longest] = (where[longest] + shift) % entries.shape[longest]
        spots.append(tuple(where))
    return entries.at[spots[0]].set(least).at[spots[1]].set(largest)


def shard_levels(key, extent, split, low, high):
    level, own = 1.0, jax.random.fold_in(key, 6)
    for dim, blocks in split:
        draws = jnp.exp(jax.random.uniform(jax.random.fold_in(own, dim), (blocks,), jnp.float32, low / len(split), high / len(split)))
        level = level * jnp.repeat(draws, extent[dim] // blocks).reshape([-1 if axis == dim else 1 for axis in range(len(extent))])
    return level


def bell_draw(rng, shape, spread, limit, shards=(), held_as=jnp.bfloat16):
    factor_of = shard_levels(rng, shape, shards, -0.22, 0.18) if shards else 1.0
    values = jax.random.normal(rng, shape, jnp.float32) * spread * factor_of
    return jnp.minimum(jnp.maximum(values, -limit), limit).astype(held_as)


def setup_inputs(seed: int = 0) -> dict:
    seeds = jax.random.split(jax.random.key(seed), 8)
    tokens = bell_draw(seeds[0], (TOKENS, D), 1.0, 6.0, ((0, 1024),))
    router = bell_draw(seeds[1], (D, EXPERTS), D ** -0.5, 0.1875)
    w_in = bell_draw(seeds[2], (EXPERTS, D, FF), D ** -0.5, 0.1875, ((0, 32),))
    w_out = bell_draw(seeds[3], (EXPERTS, FF, D), FF ** -0.5, 0.125, ((0, 32),))
    assign = draw_assign(jax.random.fold_in(seeds[7], 71), 0)
    modality = with_ends(jax.random.randint(seeds[5], (TOKENS,), 0, 2), jax.random.fold_in(seeds[5], 1), 0, 1).astype(jnp.int32)
    slot = draw_slot(jax.random.fold_in(seeds[7], 71), 0)
    return dict(tokens=tokens, router=router, w_in=w_in, w_out=w_out, assign=assign, modality=modality, slot=slot)


def expert_rows(pair):
    rows, first, second = pair
    hidden = jax.nn.gelu(jnp.dot(rows, first, preferred_element_type=jnp.float32)).astype(jnp.bfloat16)
    return jnp.dot(hidden, second, preferred_element_type=jnp.float32).astype(jnp.bfloat16)


def reference(tokens, router, w_in, w_out, assign, modality, slot):
    logits = jnp.dot(tokens, router, preferred_element_type=jnp.float32)
    probs = jax.nn.softmax(logits, axis=-1)
    logp = jax.nn.log_softmax(logits, axis=-1)
    picked = (assign[:, None] == jnp.arange(EXPERTS, dtype=jnp.int32)[None, :]).astype(jnp.float32)
    gate = jnp.sum(probs * picked, axis=-1)
    token_entropy = -jnp.sum(probs * logp, axis=-1)
    blocks = (jnp.arange(TOKENS, dtype=jnp.int32) // TOK_DEV).astype(jnp.int32)
    position = (blocks * CAP + slot).astype(jnp.int32)
    buffer = jnp.zeros((EXPERTS, DEVICES * CAP, D), jnp.bfloat16).at[assign, position].set(tokens)
    outputs = lax.map(expert_rows, (buffer, w_in, w_out))
    chosen = outputs[assign, position].astype(jnp.float32)
    mixed = (gate[:, None] * chosen).astype(jnp.bfloat16)
    kinds = (modality[:, None] == jnp.arange(2, dtype=jnp.int32)[None, :]).astype(jnp.float32)
    sums = jnp.dot(kinds.T, probs, precision=lax.Precision.HIGHEST)
    counts = jnp.sum(kinds, axis=0)
    ent_sum = jnp.dot(kinds.T, token_entropy, precision=lax.Precision.HIGHEST)
    denom = jnp.maximum(counts, 1.0)
    importance = sums / denom[:, None]
    global_ent = -jnp.sum(jax.scipy.special.xlogy(importance, importance), axis=-1)
    entropies = jnp.stack([ent_sum / denom, global_ent], axis=1)
    return mixed, importance, entropies
```

```python
import jax
import jax.numpy as jnp
from jax import lax
from jax.experimental import pallas as pl
from jax.experimental.pallas import tpu as pltpu
from jax.sharding import PartitionSpec as P

BOTH = ("dp", "expert")
F32, BF16, I32 = jnp.float32, jnp.bfloat16, jnp.int32
LANES = 128
ROWS = 8


def mm(a, b):
    return jnp.dot(a, b, preferred_element_type=F32)


def mm_t(a, b):
    return lax.dot_general(a, b, (((1,), (1,)), ((), ())), preferred_element_type=F32)


def iota(shape, dim):
    return lax.broadcasted_iota(I32, shape, dim)


def pick_labels(expert, slot):
    first = jnp.where(slot < 8, expert * 8 + slot, -1)
    low = jnp.where(slot >= 8, expert * 8 + slot - 8, -1)
    high = jnp.where(slot >= 8, expert * 8 + slot - 4, -1)
    return first, low, high


def gather_kernel(tokens, assign, slot, out):
    n_expert = out.shape[0]
    half = tokens.shape[1] // 2
    rows = n_expert * ROWS
    count = tokens.shape[0]
    experts = assign[...].reshape(1, count)
    slots = slot[...].reshape(1, count)
    first, low, high = pick_labels(experts, slots)
    row = iota((rows, count), 0)
    main = mm((first == row).astype(BF16), tokens[...]).astype(BF16)
    rest = mm((low == row).astype(BF16), tokens[:, :half])
    rest = rest + mm((high == row).astype(BF16), tokens[:, half:])
    rest = rest.astype(BF16)
    for t in range(8):
        out[:, t] = main[:, t * LANES : (t + 1) * LANES].reshape(n_expert, ROWS, LANES)
    for t in range(4):
        out[:, 8 + t] = rest[:, t * LANES : (t + 1) * LANES].reshape(n_expert, ROWS, LANES)


def split3(x):
    hi = x.astype(BF16)
    left = x - hi.astype(F32)
    mid = left.astype(BF16)
    lo = (left - mid.astype(F32)).astype(BF16)
    return hi, mid, lo


def column(row, count):
    return jnp.transpose(jnp.broadcast_to(row, (LANES, count)))


def stats_kernel(tokens, router_t, assign, modality, slot, stats, gate_out, place_first, place_low, place_high):
    n_expert, count = router_t.shape[0], tokens.shape[0]
    logits = mm_t(router_t[...], tokens[...])
    shifted = logits - jnp.max(logits, axis=0, keepdims=True)
    grown = jnp.exp(shifted)
    total = jnp.sum(grown, axis=0, keepdims=True)
    probs = grown / total
    logp = shifted - jnp.log(total)
    entropy = -jnp.sum(probs * logp, axis=0, keepdims=True)
    experts = assign[...].reshape(1, count)
    slots = slot[...].reshape(1, count)
    gate = jnp.sum(jnp.where(iota((n_expert, count), 0) == experts, probs, 0.0), axis=0, keepdims=True)
    r = iota((ROWS, count), 0)
    tail = jnp.where(r == 0, 1.0, jnp.where(r == 1, entropy, 0.0))
    pad = jnp.zeros((LANES - n_expert - ROWS, count), F32)
    terms = jnp.concatenate([probs, tail, pad], axis=0)
    kinds = (modality[...].reshape(1, count) == (iota((16, count), 0) & 1)).astype(BF16)
    hi, mid, lo = split3(terms)
    stats[...] = (mm_t(kinds, hi) + mm_t(kinds, mid) + mm_t(kinds, lo))[:ROWS]
    gate_out[...] = column(gate, count)
    wide = n_expert * ROWS
    first, low, high = pick_labels(experts, slots)
    lane = iota((count, wide), 1)

    def spread(labels):
        c = column(labels.astype(F32), count).astype(I32)
        return jnp.concatenate([c] * (wide // LANES), axis=1)

    place_first[...] = (spread(first) == lane).astype(BF16)
    place_low[...] = (spread(low) == lane).astype(BF16)
    place_high[...] = (spread(high) == lane).astype(BF16)


def ffn_kernel(received, w_in, w_out, stats, out, rows, acc):
    step = pl.program_id(0)
    n_expert = received.shape[0]
    wide = n_expert * ROWS
    quarter = wide // 2
    width = w_in.shape[1]
    half = width // 2

    @pl.when(step == 0)
    def _():
        for t in range(8):
            rows[:wide, t * LANES : (t + 1) * LANES] = received[:, t].reshape(wide, LANES)
        packed = jnp.concatenate([received[:, 8 + t].reshape(wide, LANES) for t in range(4)], axis=1)
        want = iota((quarter, wide), 0)
        have = iota((quarter, wide), 1)
        source = (want // 4) * 8 + want % 4
        rows[wide:, :half] = mm((have == source).astype(BF16), packed).astype(BF16)
        rows[wide:, half:] = mm((have == source + 4).astype(BF16), packed).astype(BF16)

    hidden = jax.nn.gelu(mm(rows[...], w_in[0])).astype(BF16)
    part = mm(hidden, w_out[0])

    @pl.when(step == 0)
    def _():
        acc[...] = part

    @pl.when(step > 0)
    def _():
        acc[...] = acc[...] + part

    @pl.when(step == pl.num_programs(0) - 1)
    def _():
        result = acc[...].astype(BF16)
        for t in range(8):
            out[:, t] = result[:wide, t * LANES : (t + 1) * LANES].reshape(n_expert, ROWS, LANES)
        want = iota((wide, quarter), 0)
        have = iota((wide, quarter), 1)
        inside = want % 8
        base = (want // 8) * 4
        low = jnp.where((inside < 4) & (have == base + inside), 1.0, 0.0).astype(BF16)
        high = jnp.where((inside >= 4) & (have == base + inside - 4), 1.0, 0.0).astype(BF16)
        packed = (mm(low, result[wide:, :half]) + mm(high, result[wide:, half:])).astype(BF16)
        for t in range(4):
            out[:, 8 + t] = packed[:, t * LANES : (t + 1) * LANES].reshape(n_expert, ROWS, LANES)
        hi, mid, lo = (p.astype(F32) for p in split3(stats[...]))
        r = iota((ROWS, LANES), 0)
        tile = jnp.where(r < 2, hi, jnp.where(r < 4, mid, jnp.where(r < 6, lo, 0.0))).astype(BF16)
        out[:, 12] = jnp.broadcast_to(tile[None], (n_expert, ROWS, LANES))


def mix_kernel(returned, gate, place_first, place_low, place_high, mixed, importance, entropies):
    n_expert = returned.shape[0]
    wide = n_expert * ROWS
    width = mixed.shape[1]
    half = width // 2
    scale = gate[...]
    scale = jnp.concatenate([scale] * (half // LANES), axis=1)
    main = jnp.concatenate([returned[:, t].reshape(wide, LANES) for t in range(8)], axis=1)
    packed = jnp.concatenate([returned[:, 8 + t].reshape(wide, LANES) for t in range(4)], axis=1)
    chosen = mm(place_first[...], main[:, :half]) + mm(place_low[...], packed)
    mixed[:, :half] = (scale * chosen).astype(BF16)
    chosen = mm(place_first[...], main[:, half:]) + mm(place_high[...], packed)
    mixed[:, half:] = (scale * chosen).astype(BF16)
    tile = jnp.sum(returned[:, 12].astype(F32), axis=0)
    total = (tile[0:2] + tile[2:4]) + tile[4:6]
    denom = jnp.maximum(total[:, n_expert : n_expert + 1], 1.0)
    mean = total[:, :n_expert] / denom
    importance[...] = mean
    terms = jnp.where(mean == 0.0, 0.0, mean * jnp.log(jnp.where(mean == 0.0, 1.0, mean)))
    spread = -jnp.sum(terms, axis=1, keepdims=True)
    token = total[:, n_expert + 1 : n_expert + 2] / denom
    entropies[...] = jnp.where(iota((2, 2), 1) == 0, token, spread)


def budget(mib):
    return pltpu.CompilerParams(vmem_limit_bytes=mib * 1024 * 1024)


def out_of(shape, dtype):
    return jax.ShapeDtypeStruct(shape, dtype)


def per_device(tokens, router, w_in, w_out, assign, modality, slot):
    count, width = tokens.shape
    n_expert = router.shape[1]
    hidden_width = w_in.shape[2]
    wide = n_expert * ROWS
    tiles = width // LANES * 3 // 2
    n_dp = lax.axis_size("dp")
    buffer = pl.pallas_call(
        gather_kernel, out_shape=out_of((n_expert, tiles, ROWS, LANES), BF16), name="gather", compiler_params=budget(24)
    )(tokens, assign, slot)
    received = lax.all_to_all(buffer, "expert", split_axis=0, concat_axis=0, tiled=True)
    stats, gate, place_first, place_low, place_high = pl.pallas_call(
        stats_kernel,
        out_shape=(
            out_of((ROWS, LANES), F32),
            out_of((count, LANES), F32),
            out_of((count, wide), BF16),
            out_of((count, wide), BF16),
            out_of((count, wide), BF16),
        ),
        name="stats",
        compiler_params=budget(24),
    )(tokens, router.T, assign, modality, slot)
    pairs = [[2 * z, 2 * z + 1] for z in range(n_dp // 2)]
    near = [[8 * j + 2 * z + c for z in range(4)] for j in range(n_dp // 8) for c in range(2)]
    far = [[8 * j + 2 * z + c for j in range(n_dp // 8)] for z in range(4) for c in range(2)]
    for groups in (pairs, near, far):
        stats = lax.psum(stats, "dp", axis_index_groups=groups)
    block = 256
    returned_in = pl.pallas_call(
        ffn_kernel,
        grid=(hidden_width // block,),
        in_specs=[
            pl.BlockSpec((n_expert, tiles, ROWS, LANES), lambda j: (0, 0, 0, 0)),
            pl.BlockSpec((1, width, block), lambda j: (0, 0, j)),
            pl.BlockSpec((1, block, width), lambda j: (0, j, 0)),
            pl.BlockSpec((ROWS, LANES), lambda j: (0, 0)),
        ],
        out_specs=pl.BlockSpec((n_expert, tiles + 1, ROWS, LANES), lambda j: (0, 0, 0, 0)),
        out_shape=out_of((n_expert, tiles + 1, ROWS, LANES), BF16),
        scratch_shapes=[
            pltpu.VMEM((wide * 3 // 2, width), BF16),
            pltpu.VMEM((wide * 3 // 2, width), F32),
        ],
        name="ffn",
        compiler_params=budget(60),
    )(received, w_in, w_out, stats)
    returned = lax.all_to_all(returned_in, "expert", split_axis=0, concat_axis=0, tiled=True)
    return pl.pallas_call(
        mix_kernel,
        out_shape=(
            out_of((count, width), BF16),
            out_of((2, n_expert), F32),
            out_of((2, 2), F32),
        ),
        name="mix",
        compiler_params=budget(24),
    )(returned, gate, place_first, place_low, place_high)


def solution(mesh):
    placed = (
        P(BOTH, None),
        P(),
        P("expert", None, None),
        P("expert", None, None),
        P(BOTH),
        P(BOTH),
        P(BOTH),
    )
    return jax.shard_map(
        per_device,
        mesh=mesh,
        in_specs=placed,
        out_specs=(P(BOTH, None), P(), P()),
        check_vma=False,
    )
```

```python
import jax
import jax.numpy as jnp
from jax import lax
from jax.experimental import pallas as pl
from jax.experimental.pallas import tpu as pltpu
from jax.sharding import PartitionSpec as P

BOTH = ("dp", "expert")
F32, BF16, I32 = jnp.float32, jnp.bfloat16, jnp.int32
LANES = 128
ROWS = 8


def mm(a, b):
    return jnp.dot(a, b, preferred_element_type=F32)


def mm_t(a, b):
    return lax.dot_general(a, b, (((1,), (1,)), ((), ())), preferred_element_type=F32)


def iota(shape, dim):
    return lax.broadcasted_iota(I32, shape, dim)


def pick_labels(expert, slot):
    first = jnp.where(slot < 8, expert * 8 + slot, -1)
    low = jnp.where(slot >= 8, expert * 8 + slot - 8, -1)
    high = jnp.where(slot >= 8, expert * 8 + slot - 4, -1)
    return first, low, high


def split3(x):
    hi = x.astype(BF16)
    left = x - hi.astype(F32)
    mid = left.astype(BF16)
    lo = (left - mid.astype(F32)).astype(BF16)
    return hi, mid, lo


def stats_tile(sums):
    hi, mid, lo = (p.astype(F32) for p in split3(sums))
    r = iota((ROWS, LANES), 0)
    return jnp.where(r < 2, hi, jnp.where(r < 4, mid, jnp.where(r < 6, lo, 0.0))).astype(BF16)


def fetch(sources, targets, sems):
    copies = [pltpu.make_async_copy(s, t, sems.at[i]) for i, (s, t) in enumerate(zip(sources, targets))]
    for c in copies:
        c.start()
    return copies


def send_kernel(
    tokens_hbm, router_hbm, assign_hbm, slot_hbm, modality_hbm, out, gate_out, tokens, router, assign, slot, modality, sems
):
    copies = fetch(
        (assign_hbm, slot_hbm, tokens_hbm, router_hbm, modality_hbm), (assign, slot, tokens, router, modality), sems
    )
    n_expert = out.shape[0]
    count, width = tokens.shape
    half = width // 2
    rows = n_expert * ROWS
    copies[0].wait()
    copies[1].wait()
    experts = assign[...].reshape(1, count)
    slots = slot[...].reshape(1, count)
    first, low, high = pick_labels(experts, slots)
    row = iota((rows, count), 0)
    pick_first = (first == row).astype(BF16)
    pick_low = (low == row).astype(BF16)
    pick_high = (high == row).astype(BF16)
    copies[2].wait()
    main = mm(pick_first, tokens[...]).astype(BF16)
    rest = mm(pick_low, tokens[:, :half]) + mm(pick_high, tokens[:, half:])
    rest = rest.astype(BF16)
    for t in range(8):
        out[:, t] = main[:, t * LANES : (t + 1) * LANES].reshape(n_expert, ROWS, LANES)
    for t in range(4):
        out[:, 8 + t] = rest[:, t * LANES : (t + 1) * LANES].reshape(n_expert, ROWS, LANES)
    copies[3].wait()
    copies[4].wait()
    logits = mm_t(router[...], tokens[...])
    shifted = logits - jnp.max(logits, axis=0, keepdims=True)
    grown = jnp.exp(shifted)
    total = jnp.sum(grown, axis=0, keepdims=True)
    probs = grown / total
    logp = shifted - jnp.log(total)
    entropy = -jnp.sum(probs * logp, axis=0, keepdims=True)
    gate = jnp.sum(jnp.where(iota((n_expert, count), 0) == experts, probs, 0.0), axis=0, keepdims=True)
    gate_out[...] = jnp.broadcast_to(gate, (ROWS, count))
    r = iota((ROWS, count), 0)
    tail = jnp.where(r == 0, 1.0, jnp.where(r == 1, entropy, 0.0))
    pad = jnp.zeros((LANES - n_expert - ROWS, count), F32)
    terms = jnp.concatenate([probs, tail, pad], axis=0)
    kinds = (modality[...].reshape(1, count) == (iota((16, count), 0) & 1)).astype(BF16)
    hi, mid, lo = split3(terms)
    sums = (mm_t(kinds, hi) + mm_t(kinds, mid) + mm_t(kinds, lo))[:ROWS]
    out[:, 12] = jnp.broadcast_to(stats_tile(sums)[None], (n_expert, ROWS, LANES))


def total_of(tiles):
    tile = jnp.sum(tiles.astype(F32), axis=0)
    return (tile[0:2] + tile[2:4]) + tile[4:6]


def group_kernel(received, group):
    total = total_of(received[:, 12])
    group[...] = jnp.concatenate([total] * (ROWS // 2), axis=0)


def fill_kernel(computed, other, out):
    n_expert = out.shape[0]
    out[:, 12] = jnp.broadcast_to(stats_tile(other[...])[None], (n_expert, ROWS, LANES))


def column(row, count):
    return jnp.transpose(jnp.broadcast_to(row, (LANES, count)))


def place_kernel(gate, assign, slot, after, gate_out, place_first, place_low, place_high):
    count = gate.shape[1]
    wide = place_first.shape[1]
    first, low, high = pick_labels(assign[...].reshape(1, count), slot[...].reshape(1, count))
    gate_out[...] = column(gate[0:1], count)
    lane = iota((count, wide), 1)

    def spread(labels):
        c = column(labels.astype(F32), count).astype(I32)
        return jnp.concatenate([c] * (wide // LANES), axis=1)

    place_first[...] = (spread(first) == lane).astype(BF16)
    place_low[...] = (spread(low) == lane).astype(BF16)
    place_high[...] = (spread(high) == lane).astype(BF16)


STEP = 256


def ffn_kernel(received, in_hbm, out_hbm, out, w_in, w_out, rows, hidden, rest, sems):
    n_expert = received.shape[0]
    wide = n_expert * ROWS
    quarter = wide // 2
    width, inner = w_in.shape
    half = width // 2
    n_in, n_out = inner // STEP, width // STEP
    order = [0, 2, 1, 3]
    cut = [pl.ds(j * STEP, STEP) for j in range(max(n_in, n_out))]
    copies = fetch(
        [in_hbm.at[0, :, cut[j]] for j in range(n_in)] + [out_hbm.at[0, :, cut[n]] for n in order],
        [w_in.at[:, cut[j]] for j in range(n_in)] + [w_out.at[:, cut[n]] for n in order],
        sems,
    )
    for t in range(8):
        rows[:wide, t * LANES : (t + 1) * LANES] = received[:, t].reshape(wide, LANES)
    packed = jnp.concatenate([received[:, 8 + t].reshape(wide, LANES) for t in range(4)], axis=1)
    want = iota((quarter, wide), 0)
    have = iota((quarter, wide), 1)
    source = (want // 4) * 8 + want % 4
    rows[wide:, :half] = mm((have == source).astype(BF16), packed).astype(BF16)
    rows[wide:, half:] = mm((have == source + 4).astype(BF16), packed).astype(BF16)
    for j in range(n_in):
        copies[j].wait()
        hidden[:, j * STEP : (j + 1) * STEP] = jax.nn.gelu(mm(rows[...], w_in[:, cut[j]])).astype(BF16)
    want = iota((wide, quarter), 0)
    have = iota((wide, quarter), 1)
    inside = want % 8
    base = (want // 8) * 4
    to_low = jnp.where((inside < 4) & (have == base + inside), 1.0, 0.0).astype(BF16)
    to_high = jnp.where((inside >= 4) & (have == base + inside - 4), 1.0, 0.0).astype(BF16)
    for i, n in enumerate(order):
        copies[n_in + i].wait()
        result = mm(hidden[...], w_out[:, cut[n]]).astype(BF16)
        for k in range(STEP // LANES):
            t = n * (STEP // LANES) + k
            out[:, t] = result[:wide, k * LANES : (k + 1) * LANES].reshape(n_expert, ROWS, LANES)
        rest[:, n * STEP : (n + 1) * STEP] = result[wide:]
        if i % 2 == 1:
            lo = order[i - 1]
            packed = mm(to_low, rest[:, lo * STEP : (lo + 1) * STEP]) + mm(to_high, rest[:, n * STEP : (n + 1) * STEP])
            packed = packed.astype(BF16)
            for k in range(STEP // LANES):
                t = 8 + lo * (STEP // LANES) + k
                out[:, t] = packed[:, k * LANES : (k + 1) * LANES].reshape(n_expert, ROWS, LANES)


def mix_kernel(returned, gate, place_first, place_low, place_high, mixed, importance, entropies):
    n_expert = returned.shape[0]
    wide = n_expert * ROWS
    width = mixed.shape[1]
    half = width // 2
    scale = gate[...]
    scale = jnp.concatenate([scale] * (half // LANES), axis=1)
    main = jnp.concatenate([returned[:, t].reshape(wide, LANES) for t in range(8)], axis=1)
    packed = jnp.concatenate([returned[:, 8 + t].reshape(wide, LANES) for t in range(4)], axis=1)
    chosen = mm(place_first[...], main[:, :half]) + mm(place_low[...], packed)
    mixed[:, :half] = (scale * chosen).astype(BF16)
    chosen = mm(place_first[...], main[:, half:]) + mm(place_high[...], packed)
    mixed[:, half:] = (scale * chosen).astype(BF16)
    total = total_of(returned[:, 12])
    denom = jnp.maximum(total[:, n_expert : n_expert + 1], 1.0)
    mean = total[:, :n_expert] / denom
    importance[...] = mean
    terms = jnp.where(mean == 0.0, 0.0, mean * jnp.log(jnp.where(mean == 0.0, 1.0, mean)))
    spread = -jnp.sum(terms, axis=1, keepdims=True)
    token = total[:, n_expert + 1 : n_expert + 2] / denom
    entropies[...] = jnp.where(iota((2, 2), 1) == 0, token, spread)


def budget(kib):
    return pltpu.CompilerParams(vmem_limit_bytes=kib * 1024)


def out_of(shape, dtype):
    return jax.ShapeDtypeStruct(shape, dtype)


HBM = pl.BlockSpec(memory_space=pltpu.HBM)
VMEM = pl.BlockSpec(memory_space=pltpu.VMEM)


def per_device(tokens, router, w_in, w_out, assign, modality, slot):
    count, width = tokens.shape
    n_expert = router.shape[1]
    inner = w_in.shape[2]
    wide = n_expert * ROWS
    tiles = width // LANES * 3 // 2
    n_dp = lax.axis_size("dp")
    block = out_of((n_expert, tiles + 1, ROWS, LANES), BF16)
    ints = pltpu.VMEM((count,), I32)
    buffer, gate = pl.pallas_call(
        send_kernel,
        in_specs=[HBM] * 5,
        out_specs=(VMEM, VMEM),
        out_shape=(block, out_of((ROWS, count), F32)),
        scratch_shapes=[
            pltpu.VMEM((count, width), BF16),
            pltpu.VMEM((n_expert, width), BF16),
            ints,
            ints,
            ints,
            pltpu.SemaphoreType.DMA((5,)),
        ],
        name="send",
        compiler_params=budget(65472),
    )(tokens, router.T, assign, slot, modality)
    received = lax.all_to_all(buffer, "expert", split_axis=0, concat_axis=0, tiled=True)
    group = pl.pallas_call(
        group_kernel, in_specs=[VMEM], out_specs=VMEM, out_shape=out_of((ROWS, LANES), F32), name="group",
        compiler_params=budget(24576),
    )(received)
    swap = [(d * n_expert + e, (d ^ e) * n_expert + e) for d in range(n_dp) for e in range(n_expert)]
    other = lax.ppermute(group, ("dp", "expert"), swap)
    computed = pl.pallas_call(
        ffn_kernel,
        in_specs=[VMEM, HBM, HBM],
        out_specs=VMEM,
        out_shape=block,
        scratch_shapes=[
            pltpu.VMEM((width, inner), BF16),
            pltpu.VMEM((inner, width), BF16),
            pltpu.VMEM((wide * 3 // 2, width), BF16),
            pltpu.VMEM((wide * 3 // 2, inner), BF16),
            pltpu.VMEM((wide // 2, width), BF16),
            pltpu.SemaphoreType.DMA((inner // STEP + width // STEP,)),
        ],
        name="ffn",
        compiler_params=budget(50000),
    )(received, w_in, w_out)
    scale, place_first, place_low, place_high = pl.pallas_call(
        place_kernel,
        in_specs=[VMEM] * 4,
        out_specs=(VMEM,) * 4,
        out_shape=(
            out_of((count, LANES), F32),
            out_of((count, wide), BF16),
            out_of((count, wide), BF16),
            out_of((count, wide), BF16),
        ),
        name="place",
        compiler_params=budget(24576),
    )(gate, assign, slot, group)
    filled = pl.pallas_call(
        fill_kernel,
        in_specs=[VMEM, VMEM],
        out_specs=VMEM,
        out_shape=block,
        input_output_aliases={0: 0},
        name="fill",
        compiler_params=budget(24576),
    )(computed, other)
    filled, scale, place_first, place_low, place_high = lax.optimization_barrier(
        (filled, scale, place_first, place_low, place_high)
    )
    returned = lax.all_to_all(filled, "expert", split_axis=0, concat_axis=0, tiled=True)
    return pl.pallas_call(
        mix_kernel,
        in_specs=[VMEM] * 5,
        out_specs=(VMEM,) * 3,
        out_shape=(
            out_of((count, width), BF16),
            out_of((2, n_expert), F32),
            out_of((2, 2), F32),
        ),
        name="mix",
        compiler_params=budget(24576),
    )(returned, scale, place_first, place_low, place_high)


def solution(mesh):
    placed = (
        P(BOTH, None),
        P(),
        P("expert", None, None),
        P("expert", None, None),
        P(BOTH),
        P(BOTH),
        P(BOTH),
    )
    return jax.shard_map(
        per_device,
        mesh=mesh,
        in_specs=placed,
        out_specs=(P(BOTH, None), P(), P()),
        check_vma=False,
    )
```

```python
import jax
import jax.numpy as jnp
from jax import lax
from jax.experimental import pallas as pl
from jax.experimental.pallas import tpu as pltpu
from jax.sharding import PartitionSpec as P

BOTH = ("dp", "expert")
F32, BF16, I32 = jnp.float32, jnp.bfloat16, jnp.int32
LANES = 128
ROWS = 8


def mm(a, b):
    return jnp.dot(a, b, preferred_element_type=F32)


def mm_t(a, b):
    return lax.dot_general(a, b, (((1,), (1,)), ((), ())), preferred_element_type=F32)


def iota(shape, dim):
    return lax.broadcasted_iota(I32, shape, dim)


def pick_labels(expert, slot):
    first = jnp.where(slot < 8, expert * 8 + slot, -1)
    low = jnp.where(slot >= 8, expert * 8 + slot - 8, -1)
    high = jnp.where(slot >= 8, expert * 8 + slot - 4, -1)
    return first, low, high


def split3(x):
    hi = x.astype(BF16)
    left = x - hi.astype(F32)
    mid = left.astype(BF16)
    lo = (left - mid.astype(F32)).astype(BF16)
    return hi, mid, lo


def stats_tile(sums):
    hi, mid, lo = (p.astype(F32) for p in split3(sums))
    r = iota((ROWS, LANES), 0)
    return jnp.where(r < 2, hi, jnp.where(r < 4, mid, jnp.where(r < 6, lo, 0.0))).astype(BF16)


def fetch(sources, targets, sems):
    copies = [pltpu.make_async_copy(s, t, sems.at[i]) for i, (s, t) in enumerate(zip(sources, targets))]
    for c in copies:
        c.start()
    return copies


def send_kernel(
    tokens_hbm, router_hbm, assign_hbm, slot_hbm, modality_hbm, out, gate_out, tokens, router, assign, slot, modality, sems
):
    copies = fetch(
        (assign_hbm, slot_hbm, tokens_hbm, router_hbm, modality_hbm), (assign, slot, tokens, router, modality), sems
    )
    n_expert = out.shape[0]
    count, width = tokens.shape
    half = width // 2
    rows = n_expert * ROWS
    copies[0].wait()
    copies[1].wait()
    experts = assign[...].reshape(1, count)
    slots = slot[...].reshape(1, count)
    first, low, high = pick_labels(experts, slots)
    row = iota((rows, count), 0)
    pick_first = (first == row).astype(BF16)
    pick_low = (low == row).astype(BF16)
    pick_high = (high == row).astype(BF16)
    copies[2].wait()
    main = mm(pick_first, tokens[...]).astype(BF16)
    rest = mm(pick_low, tokens[:, :half]) + mm(pick_high, tokens[:, half:])
    rest = rest.astype(BF16)
    for t in range(8):
        out[:, t] = main[:, t * LANES : (t + 1) * LANES].reshape(n_expert, ROWS, LANES)
    for t in range(4):
        out[:, 8 + t] = rest[:, t * LANES : (t + 1) * LANES].reshape(n_expert, ROWS, LANES)
    copies[3].wait()
    copies[4].wait()
    logits = mm_t(router[...], tokens[...])
    shifted = logits - jnp.max(logits, axis=0, keepdims=True)
    grown = jnp.exp(shifted)
    total = jnp.sum(grown, axis=0, keepdims=True)
    probs = grown / total
    logp = shifted - jnp.log(total)
    entropy = -jnp.sum(probs * logp, axis=0, keepdims=True)
    gate = jnp.sum(jnp.where(iota((n_expert, count), 0) == experts, probs, 0.0), axis=0, keepdims=True)
    gate_out[...] = jnp.broadcast_to(gate, (ROWS, count))
    r = iota((ROWS, count), 0)
    tail = jnp.where(r == 0, 1.0, jnp.where(r == 1, entropy, 0.0))
    pad = jnp.zeros((LANES - n_expert - ROWS, count), F32)
    terms = jnp.concatenate([probs, tail, pad], axis=0)
    kinds = (modality[...].reshape(1, count) == (iota((16, count), 0) & 1)).astype(BF16)
    hi, mid, lo = split3(terms)
    sums = (mm_t(kinds, hi) + mm_t(kinds, mid) + mm_t(kinds, lo))[:ROWS]
    out[:, 12] = jnp.broadcast_to(stats_tile(sums)[None], (n_expert, ROWS, LANES))


def total_of(tiles):
    tile = jnp.sum(tiles.astype(F32), axis=0)
    return (tile[0:2] + tile[2:4]) + tile[4:6]


def column(row, count):
    return jnp.transpose(jnp.broadcast_to(row, (LANES, count)))


def place_kernel(gate, assign, slot, scale, place_first, place_low, place_high):
    count = gate.shape[1]
    wide = place_first.shape[1]
    first, low, high = pick_labels(assign[...].reshape(1, count), slot[...].reshape(1, count))
    scale[...] = column(gate[0:1], count)
    lane = iota((count, wide), 1)

    def spread(labels):
        c = column(labels.astype(F32), count).astype(I32)
        return jnp.concatenate([c] * (wide // LANES), axis=1)

    place_first[...] = (spread(first) == lane).astype(BF16)
    place_low[...] = (spread(low) == lane).astype(BF16)
    place_high[...] = (spread(high) == lane).astype(BF16)


STEP = 512


def ffn_kernel(received, in_hbm, out_hbm, out, group, w_in, w_out, rows, hidden, rest, sems):
    n_expert = received.shape[0]
    wide = n_expert * ROWS
    quarter = wide // 2
    width, inner = w_in.shape
    half = width // 2
    n_in, n_out = inner // STEP, width // STEP
    cut = [pl.ds(j * STEP, STEP) for j in range(max(n_in, n_out))]
    copies = fetch(
        [in_hbm.at[0, :, cut[j]] for j in range(n_in)] + [out_hbm.at[0, :, cut[n]] for n in range(n_out)],
        [w_in.at[:, cut[j]] for j in range(n_in)] + [w_out.at[:, cut[n]] for n in range(n_out)],
        sems,
    )
    for t in range(8):
        rows[:wide, t * LANES : (t + 1) * LANES] = received[:, t].reshape(wide, LANES)
    packed = jnp.concatenate([received[:, 8 + t].reshape(wide, LANES) for t in range(4)], axis=1)
    want = iota((quarter, wide), 0)
    have = iota((quarter, wide), 1)
    source = (want // 4) * 8 + want % 4
    rows[wide:, :half] = mm((have == source).astype(BF16), packed).astype(BF16)
    rows[wide:, half:] = mm((have == source + 4).astype(BF16), packed).astype(BF16)
    total = total_of(received[:, 12])
    group[...] = jnp.concatenate([total] * (ROWS // 2), axis=0)
    for j in range(n_in):
        copies[j].wait()
        hidden[:, j * STEP : (j + 1) * STEP] = jax.nn.gelu(mm(rows[...], w_in[:, cut[j]])).astype(BF16)
    for n in range(n_out):
        copies[n_in + n].wait()
        result = mm(hidden[...], w_out[:, cut[n]]).astype(BF16)
        for k in range(STEP // LANES):
            t = n * (STEP // LANES) + k
            out[:, t] = result[:wide, k * LANES : (k + 1) * LANES].reshape(n_expert, ROWS, LANES)
        rest[:, n * STEP : (n + 1) * STEP] = result[wide:]
    want = iota((wide, quarter), 0)
    have = iota((wide, quarter), 1)
    inside = want % 8
    base = (want // 8) * 4
    to_low = jnp.where((inside < 4) & (have == base + inside), 1.0, 0.0).astype(BF16)
    to_high = jnp.where((inside >= 4) & (have == base + inside - 4), 1.0, 0.0).astype(BF16)
    packed = (mm(to_low, rest[:, :half]) + mm(to_high, rest[:, half:])).astype(BF16)
    for t in range(4):
        out[:, 8 + t] = packed[:, t * LANES : (t + 1) * LANES].reshape(n_expert, ROWS, LANES)


def mix_kernel(returned, sums, gate, place_first, place_low, place_high, mixed, importance, entropies):
    n_expert = returned.shape[0]
    wide = n_expert * ROWS
    width = mixed.shape[1]
    half = width // 2
    scale = gate[...]
    scale = jnp.concatenate([scale] * (half // LANES), axis=1)
    main = jnp.concatenate([returned[:, t].reshape(wide, LANES) for t in range(8)], axis=1)
    packed = jnp.concatenate([returned[:, 8 + t].reshape(wide, LANES) for t in range(4)], axis=1)
    chosen = mm(place_first[...], main[:, :half]) + mm(place_low[...], packed)
    mixed[:, :half] = (scale * chosen).astype(BF16)
    chosen = mm(place_first[...], main[:, half:]) + mm(place_high[...], packed)
    mixed[:, half:] = (scale * chosen).astype(BF16)
    total = sums[0:2]
    denom = jnp.maximum(total[:, n_expert : n_expert + 1], 1.0)
    mean = total[:, :n_expert] / denom
    importance[...] = mean
    terms = jnp.where(mean == 0.0, 0.0, mean * jnp.log(jnp.where(mean == 0.0, 1.0, mean)))
    spread = -jnp.sum(terms, axis=1, keepdims=True)
    token = total[:, n_expert + 1 : n_expert + 2] / denom
    entropies[...] = jnp.where(iota((2, 2), 1) == 0, token, spread)


def budget(kib):
    return pltpu.CompilerParams(vmem_limit_bytes=kib * 1024)


def out_of(shape, dtype):
    return jax.ShapeDtypeStruct(shape, dtype)


HBM = pl.BlockSpec(memory_space=pltpu.HBM)
VMEM = pl.BlockSpec(memory_space=pltpu.VMEM)


def per_device(tokens, router, w_in, w_out, assign, modality, slot):
    count, width = tokens.shape
    n_expert = router.shape[1]
    inner = w_in.shape[2]
    wide = n_expert * ROWS
    tiles = width // LANES * 3 // 2
    n_dp = lax.axis_size("dp")
    block = out_of((n_expert, tiles + 1, ROWS, LANES), BF16)
    ints = pltpu.VMEM((count,), I32)
    buffer, gate = pl.pallas_call(
        send_kernel,
        in_specs=[HBM] * 5,
        out_specs=(VMEM, VMEM),
        out_shape=(block, out_of((ROWS, count), F32)),
        scratch_shapes=[
            pltpu.VMEM((count, width), BF16),
            pltpu.VMEM((n_expert, width), BF16),
            ints,
            ints,
            ints,
            pltpu.SemaphoreType.DMA((5,)),
        ],
        name="send",
        compiler_params=budget(65472),
    )(tokens, router.T, assign, slot, modality)
    received = lax.all_to_all(buffer, "expert", split_axis=0, concat_axis=0, tiled=True)
    place = out_of((count, wide), BF16)
    scale, place_first, place_low, place_high = pl.pallas_call(
        place_kernel,
        in_specs=[VMEM] * 3,
        out_specs=(VMEM,) * 4,
        out_shape=(out_of((count, LANES), F32), place, place, place),
        name="place",
        compiler_params=budget(24576),
    )(gate, assign, slot)
    received, scale, place_first, place_low, place_high = lax.optimization_barrier(
        (received, scale, place_first, place_low, place_high)
    )
    computed, stats = pl.pallas_call(
        ffn_kernel,
        in_specs=[VMEM, HBM, HBM],
        out_specs=(VMEM, VMEM),
        out_shape=(out_of((n_expert, tiles, ROWS, LANES), BF16), out_of((ROWS, LANES), F32)),
        scratch_shapes=[
            pltpu.VMEM((width, inner), BF16),
            pltpu.VMEM((inner, width), BF16),
            pltpu.VMEM((wide * 3 // 2, width), BF16),
            pltpu.VMEM((wide * 3 // 2, inner), BF16),
            pltpu.VMEM((wide // 2, width), BF16),
            pltpu.SemaphoreType.DMA((inner // STEP + width // STEP,)),
        ],
        name="ffn",
        compiler_params=budget(50000),
    )(received, w_in, w_out)
    returned = lax.all_to_all(computed, "expert", split_axis=0, concat_axis=0, tiled=True)
    pairs = [[2 * z, 2 * z + 1] for z in range(n_dp // 2)]
    near = [[8 * j + 2 * z + c for z in range(4)] for j in range(n_dp // 8) for c in range(2)]
    far = [[8 * j + 2 * z + c for j in range(n_dp // 8)] for z in range(4) for c in range(2)]
    for groups in (pairs, near, far):
        stats = lax.psum(stats, "dp", axis_index_groups=groups)
    return pl.pallas_call(
        mix_kernel,
        in_specs=[VMEM] * 6,
        out_specs=(VMEM,) * 3,
        out_shape=(
            out_of((count, width), BF16),
            out_of((2, n_expert), F32),
            out_of((2, 2), F32),
        ),
        name="mix",
        compiler_params=budget(24576),
    )(returned, stats, scale, place_first, place_low, place_high)


def solution(mesh):
    placed = (
        P(BOTH, None),
        P(),
        P("expert", None, None),
        P("expert", None, None),
        P(BOTH),
        P(BOTH),
        P(BOTH),
    )
    return jax.shard_map(
        per_device,
        mesh=mesh,
        in_specs=placed,
        out_specs=(P(BOTH, None), P(), P()),
        check_vma=False,
    )
```

```python
import jax
import jax.numpy as jnp
from jax import lax
from jax.experimental import pallas as pl
from jax.experimental.pallas import tpu as pltpu
from jax.sharding import PartitionSpec as P

BOTH = ("dp", "expert")
F32, BF16, I32 = jnp.float32, jnp.bfloat16, jnp.int32
LANES = 128
ROWS = 8


def mm(a, b):
    return jnp.dot(a, b, preferred_element_type=F32)


def mm_t(a, b):
    return lax.dot_general(a, b, (((1,), (1,)), ((), ())), preferred_element_type=F32)


def iota(shape, dim):
    return lax.broadcasted_iota(I32, shape, dim)


def pick_labels(expert, slot):
    first = jnp.where(slot < 8, expert * 8 + slot, -1)
    low = jnp.where(slot >= 8, expert * 8 + slot - 8, -1)
    high = jnp.where(slot >= 8, expert * 8 + slot - 4, -1)
    return first, low, high


def split3(x):
    hi = x.astype(BF16)
    left = x - hi.astype(F32)
    mid = left.astype(BF16)
    lo = (left - mid.astype(F32)).astype(BF16)
    return hi, mid, lo


def stats_tile(sums):
    hi, mid, lo = (p.astype(F32) for p in split3(sums))
    r = iota((ROWS, LANES), 0)
    return jnp.where(r < 2, hi, jnp.where(r < 4, mid, jnp.where(r < 6, lo, 0.0))).astype(BF16)


def fetch(sources, targets, sems):
    copies = [pltpu.make_async_copy(s, t, sems.at[i]) for i, (s, t) in enumerate(zip(sources, targets))]
    for c in copies:
        c.start()
    return copies


def piece(source, target, start, size, sem):
    part = pl.ds(start, size)
    return pltpu.make_async_copy(source.at[:, part], target.at[:, part], sem)


def send_kernel(
    tokens_hbm, router_hbm, assign_hbm, slot_hbm, modality_hbm, out_hbm, gate_out, tokens, router, assign, slot, modality, out, sems, out_sems
):
    copies = fetch(
        (assign_hbm, slot_hbm, tokens_hbm, router_hbm, modality_hbm), (assign, slot, tokens, router, modality), sems
    )
    n_expert = out.shape[0]
    count, width = tokens.shape
    half = width // 2
    rows = n_expert * ROWS
    copies[0].wait()
    copies[1].wait()
    experts = assign[...].reshape(1, count)
    slots = slot[...].reshape(1, count)
    first, low, high = pick_labels(experts, slots)
    row = iota((rows, count), 0)
    pick_first = (first == row).astype(BF16)
    pick_low = (low == row).astype(BF16)
    pick_high = (high == row).astype(BF16)
    copies[2].wait()
    rest = mm(pick_low, tokens[:, :half]) + mm(pick_high, tokens[:, half:])
    rest = rest.astype(BF16)
    for t in range(4):
        out[:, 8 + t] = rest[:, t * LANES : (t + 1) * LANES].reshape(n_expert, ROWS, LANES)
    back = [piece(out, out_hbm, 8, 4, out_sems.at[0])]
    back[0].start()
    main = mm(pick_first, tokens[...]).astype(BF16)
    for t in range(8):
        out[:, t] = main[:, t * LANES : (t + 1) * LANES].reshape(n_expert, ROWS, LANES)
    back.append(piece(out, out_hbm, 0, 8, out_sems.at[1]))
    back[1].start()
    copies[3].wait()
    copies[4].wait()
    logits = mm_t(router[...], tokens[...])
    shifted = logits - jnp.max(logits, axis=0, keepdims=True)
    grown = jnp.exp(shifted)
    total = jnp.sum(grown, axis=0, keepdims=True)
    probs = grown / total
    logp = shifted - jnp.log(total)
    entropy = -jnp.sum(probs * logp, axis=0, keepdims=True)
    gate = jnp.sum(jnp.where(iota((n_expert, count), 0) == experts, probs, 0.0), axis=0, keepdims=True)
    gate_out[...] = jnp.broadcast_to(gate, (ROWS, count))
    r = iota((ROWS, count), 0)
    tail = jnp.where(r == 0, 1.0, jnp.where(r == 1, entropy, 0.0))
    pad = jnp.zeros((LANES - n_expert - ROWS, count), F32)
    terms = jnp.concatenate([probs, tail, pad], axis=0)
    kinds = (modality[...].reshape(1, count) == (iota((16, count), 0) & 1)).astype(BF16)
    hi, mid, lo = split3(terms)
    sums = (mm_t(kinds, hi) + mm_t(kinds, mid) + mm_t(kinds, lo))[:ROWS]
    out[:, 12] = jnp.broadcast_to(stats_tile(sums)[None], (n_expert, ROWS, LANES))
    back.append(piece(out, out_hbm, 12, 1, out_sems.at[2]))
    back[2].start()
    for c in back:
        c.wait()


def total_of(tiles):
    tile = jnp.sum(tiles.astype(F32), axis=0)
    return (tile[0:2] + tile[2:4]) + tile[4:6]


def column(row, count):
    return jnp.transpose(jnp.broadcast_to(row, (LANES, count)))


EARLY = 768


def place_kernel(gate, assign, slot, in_hbm, scale, place_first, place_low, place_high, early, sem):
    ahead = pltpu.make_async_copy(in_hbm.at[0, :, pl.ds(0, EARLY)], early, sem)
    ahead.start()
    count = gate.shape[1]
    wide = place_first.shape[1]
    first, low, high = pick_labels(assign[...].reshape(1, count), slot[...].reshape(1, count))
    scale[...] = column(gate[0:1], count)
    lane = iota((count, wide), 1)

    def spread(labels):
        c = column(labels.astype(F32), count).astype(I32)
        return jnp.concatenate([c] * (wide // LANES), axis=1)

    place_first[...] = (spread(first) == lane).astype(BF16)
    place_low[...] = (spread(low) == lane).astype(BF16)
    place_high[...] = (spread(high) == lane).astype(BF16)
    ahead.wait()


STEP = 512


def ffn_kernel(received, early, in_hbm, out_hbm, back_hbm, group, w_in, w_out, rows, hidden, rest, out, sems, back_sems):
    n_expert = received.shape[0]
    wide = n_expert * ROWS
    quarter = wide // 2
    inner, width = w_out.shape
    half = width // 2
    edges = list(range(EARLY, inner, STEP)) + [inner]
    if edges[-1] - edges[-2] < STEP:
        edges.pop(-2)
    cuts = [pl.ds(lo, hi - lo) for lo, hi in zip(edges, edges[1:])]
    halves = [pl.ds(0, half), pl.ds(half, half)]
    copies = fetch(
        [in_hbm.at[0, :, c] for c in cuts] + [out_hbm.at[0, :, c] for c in halves],
        [w_in.at[:, pl.ds(c.start - EARLY, c.size)] for c in cuts] + [w_out.at[:, c] for c in halves],
        sems,
    )
    for t in range(8):
        rows[:wide, t * LANES : (t + 1) * LANES] = received[:, t].reshape(wide, LANES)
    packed = jnp.concatenate([received[:, 8 + t].reshape(wide, LANES) for t in range(4)], axis=1)
    want = iota((quarter, wide), 0)
    have = iota((quarter, wide), 1)
    source = (want // 4) * 8 + want % 4
    rows[wide:, :half] = mm((have == source).astype(BF16), packed).astype(BF16)
    rows[wide:, half:] = mm((have == source + 4).astype(BF16), packed).astype(BF16)
    total = total_of(received[:, 12])
    group[...] = jnp.concatenate([total] * (ROWS // 2), axis=0)
    for lo in range(0, EARLY, STEP):
        hi = min(lo + STEP, EARLY)
        hidden[:, lo:hi] = jax.nn.gelu(mm(rows[...], early[:, lo:hi])).astype(BF16)
    for j, c in enumerate(cuts):
        copies[j].wait()
        lo, hi = c.start, c.start + c.size
        hidden[:, lo:hi] = jax.nn.gelu(mm(rows[...], w_in[:, lo - EARLY : hi - EARLY])).astype(BF16)
    back = []
    for n, c in enumerate(halves):
        copies[len(cuts) + n].wait()
        result = mm(hidden[...], w_out[:, c]).astype(BF16)
        for k in range(half // LANES):
            out[:, 4 * n + k] = result[:wide, k * LANES : (k + 1) * LANES].reshape(n_expert, ROWS, LANES)
        rest[:, n * half : (n + 1) * half] = result[wide:]
        back.append(piece(out, back_hbm, 4 * n, 4, back_sems.at[n]))
        back[n].start()
    want = iota((wide, quarter), 0)
    have = iota((wide, quarter), 1)
    inside = want % 8
    base = (want // 8) * 4
    to_low = jnp.where((inside < 4) & (have == base + inside), 1.0, 0.0).astype(BF16)
    to_high = jnp.where((inside >= 4) & (have == base + inside - 4), 1.0, 0.0).astype(BF16)
    packed = (mm(to_low, rest[:, :half]) + mm(to_high, rest[:, half:])).astype(BF16)
    for t in range(4):
        out[:, 8 + t] = packed[:, t * LANES : (t + 1) * LANES].reshape(n_expert, ROWS, LANES)
    back.append(piece(out, back_hbm, 8, 4, back_sems.at[2]))
    back[2].start()
    for c in back:
        c.wait()


def mix_kernel(returned, sums, gate, place_first, place_low, place_high, mixed_hbm, importance, entropies, mixed, sems):
    n_expert = returned.shape[0]
    wide = n_expert * ROWS
    width = mixed.shape[1]
    half = width // 2
    scale = gate[...]
    scale = jnp.concatenate([scale] * (half // LANES), axis=1)
    main = jnp.concatenate([returned[:, t].reshape(wide, LANES) for t in range(8)], axis=1)
    packed = jnp.concatenate([returned[:, 8 + t].reshape(wide, LANES) for t in range(4)], axis=1)
    chosen = mm(place_first[...], main[:, :half]) + mm(place_low[...], packed)
    mixed[:, :half] = (scale * chosen).astype(BF16)
    cuts = [pl.ds(0, half), pl.ds(half, half)]
    back = [pltpu.make_async_copy(mixed.at[:, c], mixed_hbm.at[:, c], sems.at[i]) for i, c in enumerate(cuts)]
    back[0].start()
    chosen = mm(place_first[...], main[:, half:]) + mm(place_high[...], packed)
    mixed[:, half:] = (scale * chosen).astype(BF16)
    back[1].start()
    total = sums[0:2]
    denom = jnp.maximum(total[:, n_expert : n_expert + 1], 1.0)
    mean = total[:, :n_expert] / denom
    importance[...] = mean
    terms = jnp.where(mean == 0.0, 0.0, mean * jnp.log(jnp.where(mean == 0.0, 1.0, mean)))
    spread = -jnp.sum(terms, axis=1, keepdims=True)
    token = total[:, n_expert + 1 : n_expert + 2] / denom
    entropies[...] = jnp.where(iota((2, 2), 1) == 0, token, spread)
    for c in back:
        c.wait()


def budget(kib):
    return pltpu.CompilerParams(vmem_limit_bytes=kib * 1024)


def out_of(shape, dtype):
    return jax.ShapeDtypeStruct(shape, dtype)


HBM = pl.BlockSpec(memory_space=pltpu.HBM)
VMEM = pl.BlockSpec(memory_space=pltpu.VMEM)


def per_device(tokens, router, w_in, w_out, assign, modality, slot):
    count, width = tokens.shape
    n_expert = router.shape[1]
    inner = w_in.shape[2]
    wide = n_expert * ROWS
    tiles = width // LANES * 3 // 2
    n_dp = lax.axis_size("dp")
    block = out_of((n_expert, tiles + 1, ROWS, LANES), BF16)
    ints = pltpu.VMEM((count,), I32)
    buffer, gate = pl.pallas_call(
        send_kernel,
        in_specs=[HBM] * 5,
        out_specs=(HBM, VMEM),
        out_shape=(block, out_of((ROWS, count), F32)),
        scratch_shapes=[
            pltpu.VMEM((count, width), BF16),
            pltpu.VMEM((n_expert, width), BF16),
            ints,
            ints,
            ints,
            pltpu.VMEM((n_expert, tiles + 1, ROWS, LANES), BF16),
            pltpu.SemaphoreType.DMA((5,)),
            pltpu.SemaphoreType.DMA((3,)),
        ],
        name="send",
        compiler_params=budget(65472),
    )(tokens, router.T, assign, slot, modality)
    received = lax.all_to_all(buffer, "expert", split_axis=0, concat_axis=0, tiled=True)
    place = out_of((count, wide), BF16)
    scale, place_first, place_low, place_high, early = pl.pallas_call(
        place_kernel,
        in_specs=[VMEM] * 3 + [HBM],
        out_specs=(VMEM,) * 5,
        out_shape=(out_of((count, LANES), F32), place, place, place, out_of((width, EARLY), BF16)),
        scratch_shapes=[pltpu.SemaphoreType.DMA(())],
        name="place",
        compiler_params=budget(24576),
    )(gate, assign, slot, w_in)
    computed, stats = pl.pallas_call(
        ffn_kernel,
        in_specs=[VMEM, VMEM, HBM, HBM],
        out_specs=(HBM, VMEM),
        out_shape=(out_of((n_expert, tiles, ROWS, LANES), BF16), out_of((ROWS, LANES), F32)),
        scratch_shapes=[
            pltpu.VMEM((width, inner - EARLY), BF16),
            pltpu.VMEM((inner, width), BF16),
            pltpu.VMEM((wide * 3 // 2, width), BF16),
            pltpu.VMEM((wide * 3 // 2, inner), BF16),
            pltpu.VMEM((wide // 2, width), BF16),
            pltpu.VMEM((n_expert, tiles, ROWS, LANES), BF16),
            pltpu.SemaphoreType.DMA((8,)),
            pltpu.SemaphoreType.DMA((3,)),
        ],
        name="ffn",
        compiler_params=budget(50000),
    )(received, early, w_in, w_out)
    returned = lax.all_to_all(computed, "expert", split_axis=0, concat_axis=0, tiled=True)
    pairs = [[2 * z, 2 * z + 1] for z in range(n_dp // 2)]
    near = [[8 * j + 2 * z + c for z in range(4)] for j in range(n_dp // 8) for c in range(2)]
    far = [[8 * j + 2 * z + c for j in range(n_dp // 8)] for z in range(4) for c in range(2)]
    for groups in (pairs, near, far):
        stats = lax.psum(stats, "dp", axis_index_groups=groups)
    return pl.pallas_call(
        mix_kernel,
        in_specs=[VMEM] * 6,
        out_specs=(HBM, VMEM, VMEM),
        out_shape=(
            out_of((count, width), BF16),
            out_of((2, n_expert), F32),
            out_of((2, 2), F32),
        ),
        scratch_shapes=[pltpu.VMEM((count, width), BF16), pltpu.SemaphoreType.DMA((2,))],
        name="mix",
        compiler_params=budget(24576),
    )(returned, stats, scale, place_first, place_low, place_high)


def solution(mesh):
    placed = (
        P(BOTH, None),
        P(),
        P("expert", None, None),
        P("expert", None, None),
        P(BOTH),
        P(BOTH),
        P(BOTH),
    )
    return jax.shard_map(
        per_device,
        mesh=mesh,
        in_specs=placed,
        out_specs=(P(BOTH, None), P(), P()),
        check_vma=False,
    )
```

```python
import jax
import jax.numpy as jnp
from jax import lax
from jax.experimental import pallas as pl
from jax.experimental.pallas import tpu as pltpu
from jax.sharding import PartitionSpec as P


BOTH = ("dp", "expert")
F32, BF16, I32 = jnp.float32, jnp.bfloat16, jnp.int32
LANES = 128
ROWS = 8


def mm(a, b):
    return jnp.dot(a, b, preferred_element_type=F32)


def mm_t(a, b):
    return lax.dot_general(a, b, (((1,), (1,)), ((), ())), preferred_element_type=F32)


def iota(shape, dim):
    return lax.broadcasted_iota(I32, shape, dim)


def pick_labels(expert, slot):
    first = jnp.where(slot < 8, expert * 8 + slot, -1)
    low = jnp.where(slot >= 8, expert * 8 + slot - 8, -1)
    high = jnp.where(slot >= 8, expert * 8 + slot - 4, -1)
    return first, low, high


def split3(x):
    hi = x.astype(BF16)
    left = x - hi.astype(F32)
    mid = left.astype(BF16)
    lo = (left - mid.astype(F32)).astype(BF16)
    return hi, mid, lo


def stats_tile(sums):
    hi, mid, lo = (p.astype(F32) for p in split3(sums))
    r = iota((ROWS, LANES), 0)
    return jnp.where(r < 2, hi, jnp.where(r < 4, mid, jnp.where(r < 6, lo, 0.0))).astype(BF16)


def fetch(sources, targets, sems):
    copies = [pltpu.make_async_copy(s, t, sems.at[i]) for i, (s, t) in enumerate(zip(sources, targets))]
    for c in copies:
        c.start()
    return copies


def piece(source, target, start, size, sem):
    part = pl.ds(start, size)
    return pltpu.make_async_copy(source.at[:, part], target.at[:, part], sem)


def send_kernel(
    tokens_hbm, router_hbm, assign_hbm, slot_hbm, modality_hbm, out, gate_out, tokens, router, assign, slot, modality, sems
):
    copies = fetch(
        (assign_hbm, slot_hbm, tokens_hbm, router_hbm, modality_hbm), (assign, slot, tokens, router, modality), sems
    )
    n_expert = out.shape[0]
    count, width = tokens.shape
    half = width // 2
    rows = n_expert * ROWS
    copies[0].wait()
    copies[1].wait()
    experts = assign[...].reshape(1, count)
    slots = slot[...].reshape(1, count)
    first, low, high = pick_labels(experts, slots)
    row = iota((rows, count), 0)
    pick_first = (first == row).astype(BF16)
    pick_low = (low == row).astype(BF16)
    pick_high = (high == row).astype(BF16)
    copies[2].wait()
    main = mm(pick_first, tokens[...]).astype(BF16)
    rest = mm(pick_low, tokens[:, :half]) + mm(pick_high, tokens[:, half:])
    rest = rest.astype(BF16)
    for t in range(8):
        out[:, t] = main[:, t * LANES : (t + 1) * LANES].reshape(n_expert, ROWS, LANES)
    for t in range(4):
        out[:, 8 + t] = rest[:, t * LANES : (t + 1) * LANES].reshape(n_expert, ROWS, LANES)
    copies[3].wait()
    copies[4].wait()
    logits = mm_t(router[...], tokens[...])
    shifted = logits - jnp.max(logits, axis=0, keepdims=True)
    grown = jnp.exp(shifted)
    total = jnp.sum(grown, axis=0, keepdims=True)
    probs = grown / total
    logp = shifted - jnp.log(total)
    entropy = -jnp.sum(probs * logp, axis=0, keepdims=True)
    gate = jnp.sum(jnp.where(iota((n_expert, count), 0) == experts, probs, 0.0), axis=0, keepdims=True)
    gate_out[...] = jnp.broadcast_to(gate, (ROWS, count))
    r = iota((ROWS, count), 0)
    tail = jnp.where(r == 0, 1.0, jnp.where(r == 1, entropy, 0.0))
    pad = jnp.zeros((LANES - n_expert - ROWS, count), F32)
    terms = jnp.concatenate([probs, tail, pad], axis=0)
    kinds = (modality[...].reshape(1, count) == (iota((16, count), 0) & 1)).astype(BF16)
    hi, mid, lo = split3(terms)
    sums = (mm_t(kinds, hi) + mm_t(kinds, mid) + mm_t(kinds, lo))[:ROWS]
    out[:, 12] = jnp.broadcast_to(stats_tile(sums)[None], (n_expert, ROWS, LANES))


def total_of(tiles):
    tile = jnp.sum(tiles.astype(F32), axis=0)
    return (tile[0:2] + tile[2:4]) + tile[4:6]


def group_kernel(received, group):
    total = total_of(received[:, 12])
    group[...] = jnp.concatenate([total] * (ROWS // 2), axis=0)


def column(row, count):
    return jnp.transpose(jnp.broadcast_to(row, (LANES, count)))


EARLY = 768


def place_kernel(gate, assign, slot, in_hbm, scale, place_first, place_low, place_high, early, sem):
    ahead = pltpu.make_async_copy(in_hbm.at[0, :, pl.ds(0, EARLY)], early, sem)
    ahead.start()
    count = gate.shape[1]
    wide = place_first.shape[1]
    first, low, high = pick_labels(assign[...].reshape(1, count), slot[...].reshape(1, count))
    scale[...] = column(gate[0:1], count)
    lane = iota((count, wide), 1)

    def spread(labels):
        c = column(labels.astype(F32), count).astype(I32)
        return jnp.concatenate([c] * (wide // LANES), axis=1)

    place_first[...] = (spread(first) == lane).astype(BF16)
    place_low[...] = (spread(low) == lane).astype(BF16)
    place_high[...] = (spread(high) == lane).astype(BF16)
    ahead.wait()


STEP = 512


def ffn_kernel(received, early, in_hbm, out_hbm, back_hbm, w_in, w_out, rows, hidden, rest, out, sems, back_sems):
    n_expert = received.shape[0]
    wide = n_expert * ROWS
    quarter = wide // 2
    inner, width = w_out.shape
    half = width // 2
    edges = list(range(EARLY, inner, STEP)) + [inner]
    if edges[-1] - edges[-2] < STEP:
        edges.pop(-2)
    cuts = [pl.ds(lo, hi - lo) for lo, hi in zip(edges, edges[1:])]
    halves = [pl.ds(0, half), pl.ds(half, half)]
    copies = fetch(
        [in_hbm.at[0, :, c] for c in cuts] + [out_hbm.at[0, :, c] for c in halves],
        [w_in.at[:, pl.ds(c.start - EARLY, c.size)] for c in cuts] + [w_out.at[:, c] for c in halves],
        sems,
    )
    for t in range(8):
        rows[:wide, t * LANES : (t + 1) * LANES] = received[:, t].reshape(wide, LANES)
    packed = jnp.concatenate([received[:, 8 + t].reshape(wide, LANES) for t in range(4)], axis=1)
    want = iota((quarter, wide), 0)
    have = iota((quarter, wide), 1)
    source = (want // 4) * 8 + want % 4
    rows[wide:, :half] = mm((have == source).astype(BF16), packed).astype(BF16)
    rows[wide:, half:] = mm((have == source + 4).astype(BF16), packed).astype(BF16)
    for lo in range(0, EARLY, STEP):
        hi = min(lo + STEP, EARLY)
        hidden[:, lo:hi] = jax.nn.gelu(mm(rows[...], early[:, lo:hi])).astype(BF16)
    for j, c in enumerate(cuts):
        copies[j].wait()
        lo, hi = c.start, c.start + c.size
        hidden[:, lo:hi] = jax.nn.gelu(mm(rows[...], w_in[:, lo - EARLY : hi - EARLY])).astype(BF16)
    back = []
    for n, c in enumerate(halves):
        copies[len(cuts) + n].wait()
        result = mm(hidden[...], w_out[:, c]).astype(BF16)
        for k in range(half // LANES):
            out[:, 4 * n + k] = result[:wide, k * LANES : (k + 1) * LANES].reshape(n_expert, ROWS, LANES)
        rest[:, n * half : (n + 1) * half] = result[wide:]
        back.append(piece(out, back_hbm, 4 * n, 4, back_sems.at[n]))
        back[n].start()
    want = iota((wide, quarter), 0)
    have = iota((wide, quarter), 1)
    inside = want % 8
    base = (want // 8) * 4
    to_low = jnp.where((inside < 4) & (have == base + inside), 1.0, 0.0).astype(BF16)
    to_high = jnp.where((inside >= 4) & (have == base + inside - 4), 1.0, 0.0).astype(BF16)
    packed = (mm(to_low, rest[:, :half]) + mm(to_high, rest[:, half:])).astype(BF16)
    for t in range(4):
        out[:, 8 + t] = packed[:, t * LANES : (t + 1) * LANES].reshape(n_expert, ROWS, LANES)
    back.append(piece(out, back_hbm, 8, 4, back_sems.at[2]))
    back[2].start()
    for c in back:
        c.wait()


def mix_kernel(returned, sums, gate, place_first, place_low, place_high, mixed, importance, entropies):
    n_expert = returned.shape[0]
    wide = n_expert * ROWS
    width = mixed.shape[1]
    half = width // 2
    scale = gate[...]
    scale = jnp.concatenate([scale] * (half // LANES), axis=1)
    main = jnp.concatenate([returned[:, t].reshape(wide, LANES) for t in range(8)], axis=1)
    packed = jnp.concatenate([returned[:, 8 + t].reshape(wide, LANES) for t in range(4)], axis=1)
    chosen = mm(place_first[...], main[:, :half]) + mm(place_low[...], packed)
    mixed[:, :half] = (scale * chosen).astype(BF16)
    chosen = mm(place_first[...], main[:, half:]) + mm(place_high[...], packed)
    mixed[:, half:] = (scale * chosen).astype(BF16)
    total = sums[0:2]
    denom = jnp.maximum(total[:, n_expert : n_expert + 1], 1.0)
    mean = total[:, :n_expert] / denom
    importance[...] = mean
    terms = jnp.where(mean == 0.0, 0.0, mean * jnp.log(jnp.where(mean == 0.0, 1.0, mean)))
    spread = -jnp.sum(terms, axis=1, keepdims=True)
    token = total[:, n_expert + 1 : n_expert + 2] / denom
    entropies[...] = jnp.where(iota((2, 2), 1) == 0, token, spread)


def budget(kib):
    return pltpu.CompilerParams(vmem_limit_bytes=kib * 1024)


def out_of(shape, dtype):
    return jax.ShapeDtypeStruct(shape, dtype)


HBM = pl.BlockSpec(memory_space=pltpu.HBM)
VMEM = pl.BlockSpec(memory_space=pltpu.VMEM)


def per_device(tokens, router, w_in, w_out, assign, modality, slot):
    count, width = tokens.shape
    n_expert = router.shape[1]
    inner = w_in.shape[2]
    wide = n_expert * ROWS
    tiles = width // LANES * 3 // 2
    n_dp = lax.axis_size("dp")
    block = out_of((n_expert, tiles + 1, ROWS, LANES), BF16)
    ints = pltpu.VMEM((count,), I32)
    buffer, gate = pl.pallas_call(
        send_kernel,
        in_specs=[HBM] * 5,
        out_specs=(VMEM, VMEM),
        out_shape=(block, out_of((ROWS, count), F32)),
        scratch_shapes=[
            pltpu.VMEM((count, width), BF16),
            pltpu.VMEM((n_expert, width), BF16),
            ints,
            ints,
            ints,
            pltpu.SemaphoreType.DMA((5,)),
        ],
        name="send",
        compiler_params=budget(65472),
    )(tokens, router.T, assign, slot, modality)
    received = lax.all_to_all(buffer, "expert", split_axis=0, concat_axis=0, tiled=True)
    place = out_of((count, wide), BF16)
    scale, place_first, place_low, place_high, early = pl.pallas_call(
        place_kernel,
        in_specs=[VMEM] * 3 + [HBM],
        out_specs=(VMEM,) * 5,
        out_shape=(out_of((count, LANES), F32), place, place, place, out_of((width, EARLY), BF16)),
        scratch_shapes=[pltpu.SemaphoreType.DMA(())],
        name="place",
        compiler_params=budget(24576),
    )(gate, assign, slot, w_in)
    stats = pl.pallas_call(
        group_kernel,
        in_specs=[VMEM],
        out_specs=VMEM,
        out_shape=out_of((ROWS, LANES), F32),
        name="group",
        compiler_params=budget(24576),
    )(received)
    other = lax.ppermute(stats, "dp", [(d, d ^ 4) for d in range(n_dp)])
    matmuls = pl.pallas_call(
        ffn_kernel,
        in_specs=[VMEM, VMEM, HBM, HBM],
        out_specs=HBM,
        out_shape=out_of((n_expert, tiles, ROWS, LANES), BF16),
        scratch_shapes=[
            pltpu.VMEM((width, inner - EARLY), BF16),
            pltpu.VMEM((inner, width), BF16),
            pltpu.VMEM((wide * 3 // 2, width), BF16),
            pltpu.VMEM((wide * 3 // 2, inner), BF16),
            pltpu.VMEM((wide // 2, width), BF16),
            pltpu.VMEM((n_expert, tiles, ROWS, LANES), BF16),
            pltpu.SemaphoreType.DMA((8,)),
            pltpu.SemaphoreType.DMA((3,)),
        ],
        name="ffn",
        compiler_params=budget(50000),
    )
    computed = matmuls(received, early, w_in, w_out)
    returned = lax.all_to_all(computed, "expert", split_axis=0, concat_axis=0, tiled=True)
    near = [[4 * j + i for i in range(4)] for j in range(n_dp // 4)]
    far = [[8 * j + i for j in range(n_dp // 8)] for i in range(8)]
    stats = stats + other
    for groups in (near, far):
        stats = lax.psum(stats, "dp", axis_index_groups=groups)
    return pl.pallas_call(
        mix_kernel,
        in_specs=[VMEM] * 6,
        out_specs=(VMEM,) * 3,
        out_shape=(
            out_of((count, width), BF16),
            out_of((2, n_expert), F32),
            out_of((2, 2), F32),
        ),
        name="mix",
        compiler_params=budget(24576),
    )(returned, stats, scale, place_first, place_low, place_high)


def solution(mesh):
    placed = (
        P(BOTH, None),
        P(),
        P("expert", None, None),
        P("expert", None, None),
        P(BOTH),
        P(BOTH),
        P(BOTH),
    )
    return jax.shard_map(
        per_device,
        mesh=mesh,
        in_specs=placed,
        out_specs=(P(BOTH, None), P(), P()),
        check_vma=False,
    )
```

```python
import jax
import jax.numpy as jnp
from jax import lax
from jax.experimental import pallas as pl
from jax.experimental.pallas import tpu as pltpu
from jax.sharding import PartitionSpec as P


BOTH = ("dp", "expert")
F32, BF16, I32 = jnp.float32, jnp.bfloat16, jnp.int32
LANES = 128
ROWS = 8


def mm(a, b):
    return jnp.dot(a, b, preferred_element_type=F32)


def mm_t(a, b):
    return lax.dot_general(a, b, (((1,), (1,)), ((), ())), preferred_element_type=F32)


def iota(shape, dim):
    return lax.broadcasted_iota(I32, shape, dim)


def pick_labels(expert, slot):
    first = jnp.where(slot < 8, expert * 8 + slot, -1)
    low = jnp.where(slot >= 8, expert * 8 + slot - 8, -1)
    high = jnp.where(slot >= 8, expert * 8 + slot - 4, -1)
    return first, low, high


def split3(x):
    hi = x.astype(BF16)
    left = x - hi.astype(F32)
    mid = left.astype(BF16)
    lo = (left - mid.astype(F32)).astype(BF16)
    return hi, mid, lo


def stats_tile(sums):
    hi, mid, lo = (p.astype(F32) for p in split3(sums))
    r = iota((ROWS, LANES), 0)
    return jnp.where(r < 2, hi, jnp.where(r < 4, mid, jnp.where(r < 6, lo, 0.0))).astype(BF16)


def fetch(sources, targets, sems):
    copies = [pltpu.make_async_copy(s, t, sems.at[i]) for i, (s, t) in enumerate(zip(sources, targets))]
    for c in copies:
        c.start()
    return copies


def piece(source, target, start, size, sem):
    part = pl.ds(start, size)
    return pltpu.make_async_copy(source.at[:, part], target.at[:, part], sem)


def send_kernel(
    tokens_hbm, router_hbm, assign_hbm, slot_hbm, modality_hbm, out, gate_out, tokens, router, assign, slot, modality, sems
):
    copies = fetch(
        (assign_hbm, slot_hbm, tokens_hbm, router_hbm, modality_hbm), (assign, slot, tokens, router, modality), sems
    )
    n_expert = out.shape[0]
    count, width = tokens.shape
    half = width // 2
    rows = n_expert * ROWS
    for i in (0, 1, 3, 4):
        copies[i].wait()
    experts = assign[...].reshape(1, count)
    slots = slot[...].reshape(1, count)
    first, low, high = pick_labels(experts, slots)
    row = iota((rows, count), 0)
    pick_first = (first == row).astype(BF16)
    pick_low = (low == row).astype(BF16)
    pick_high = (high == row).astype(BF16)
    copies[2].wait()
    main = mm(pick_first, tokens[...]).astype(BF16)
    rest = mm(pick_low, tokens[:, :half]) + mm(pick_high, tokens[:, half:])
    rest = rest.astype(BF16)
    for t in range(8):
        out[:, t] = main[:, t * LANES : (t + 1) * LANES].reshape(n_expert, ROWS, LANES)
    for t in range(4):
        out[:, 8 + t] = rest[:, t * LANES : (t + 1) * LANES].reshape(n_expert, ROWS, LANES)
    logits = mm_t(router[...], tokens[...])
    shifted = logits - jnp.max(logits, axis=0, keepdims=True)
    grown = jnp.exp(shifted)
    total = jnp.sum(grown, axis=0, keepdims=True)
    probs = grown / total
    logp = shifted - jnp.log(total)
    entropy = -jnp.sum(probs * logp, axis=0, keepdims=True)
    gate = jnp.sum(jnp.where(iota((n_expert, count), 0) == experts, probs, 0.0), axis=0, keepdims=True)
    gate_out[...] = jnp.broadcast_to(gate, (ROWS, count))
    r = iota((ROWS, count), 0)
    tail = jnp.where(r == 0, 1.0, jnp.where(r == 1, entropy, 0.0))
    pad = jnp.zeros((LANES - n_expert - ROWS, count), F32)
    terms = jnp.concatenate([probs, tail, pad], axis=0)
    kinds = (modality[...].reshape(1, count) == (iota((16, count), 0) & 1)).astype(BF16)
    hi, mid, lo = split3(terms)
    sums = (mm_t(kinds, hi) + mm_t(kinds, mid) + mm_t(kinds, lo))[:ROWS]
    out[:, 12] = jnp.broadcast_to(stats_tile(sums)[None], (n_expert, ROWS, LANES))


def total_of(tiles):
    tile = jnp.sum(tiles.astype(F32), axis=0)
    return (tile[0:2] + tile[2:4]) + tile[4:6]


def group_kernel(received, group):
    total = total_of(received[:, 12])
    group[...] = jnp.concatenate([total] * (ROWS // 2), axis=0)


def column(row, count):
    return jnp.transpose(jnp.broadcast_to(row, (LANES, count)))


EARLY = 768


def place_kernel(gate, assign, slot, in_hbm, scale, place_first, place_low, place_high, early, sem):
    ahead = pltpu.make_async_copy(in_hbm.at[0, :, pl.ds(0, EARLY)], early, sem)
    ahead.start()
    count = gate.shape[1]
    wide = place_first.shape[1]
    first, low, high = pick_labels(assign[...].reshape(1, count), slot[...].reshape(1, count))
    scale[...] = column(gate[0:1], count)
    lane = iota((count, wide), 1)

    def spread(labels):
        c = column(labels.astype(F32), count).astype(I32)
        return jnp.concatenate([c] * (wide // LANES), axis=1)

    place_first[...] = (spread(first) == lane).astype(BF16)
    place_low[...] = (spread(low) == lane).astype(BF16)
    place_high[...] = (spread(high) == lane).astype(BF16)
    ahead.wait()


STEP = 512


def ffn_kernel(received, early, in_hbm, out_hbm, back_hbm, w_in, w_out, rows, hidden, rest, out, sems, back_sems):
    n_expert = received.shape[0]
    wide = n_expert * ROWS
    quarter = wide // 2
    inner, width = w_out.shape
    half = width // 2
    edges = list(range(EARLY, inner, STEP)) + [inner]
    if edges[-1] - edges[-2] < STEP:
        edges.pop(-2)
    cuts = [pl.ds(lo, hi - lo) for lo, hi in zip(edges, edges[1:])]
    halves = [pl.ds(0, half), pl.ds(half, half)]
    copies = fetch(
        [in_hbm.at[0, :, c] for c in cuts] + [out_hbm.at[0, :, c] for c in halves],
        [w_in.at[:, pl.ds(c.start - EARLY, c.size)] for c in cuts] + [w_out.at[:, c] for c in halves],
        sems,
    )
    for t in range(8):
        rows[:wide, t * LANES : (t + 1) * LANES] = received[:, t].reshape(wide, LANES)
    packed = jnp.concatenate([received[:, 8 + t].reshape(wide, LANES) for t in range(4)], axis=1)
    want = iota((quarter, wide), 0)
    have = iota((quarter, wide), 1)
    source = (want // 4) * 8 + want % 4
    rows[wide:, :half] = mm((have == source).astype(BF16), packed).astype(BF16)
    rows[wide:, half:] = mm((have == source + 4).astype(BF16), packed).astype(BF16)
    for lo in range(0, EARLY, STEP):
        hi = min(lo + STEP, EARLY)
        hidden[:, lo:hi] = jax.nn.gelu(mm(rows[...], early[:, lo:hi])).astype(BF16)
    for j, c in enumerate(cuts):
        copies[j].wait()
        lo, hi = c.start, c.start + c.size
        hidden[:, lo:hi] = jax.nn.gelu(mm(rows[...], w_in[:, lo - EARLY : hi - EARLY])).astype(BF16)
    back = []
    for n, c in enumerate(halves):
        copies[len(cuts) + n].wait()
        result = mm(hidden[...], w_out[:, c]).astype(BF16)
        for k in range(half // LANES):
            out[:, 4 * n + k] = result[:wide, k * LANES : (k + 1) * LANES].reshape(n_expert, ROWS, LANES)
        rest[:, n * half : (n + 1) * half] = result[wide:]
        back.append(piece(out, back_hbm, 4 * n, 4, back_sems.at[n]))
        back[n].start()
    want = iota((wide, quarter), 0)
    have = iota((wide, quarter), 1)
    inside = want % 8
    base = (want // 8) * 4
    to_low = jnp.where((inside < 4) & (have == base + inside), 1.0, 0.0).astype(BF16)
    to_high = jnp.where((inside >= 4) & (have == base + inside - 4), 1.0, 0.0).astype(BF16)
    packed = (mm(to_low, rest[:, :half]) + mm(to_high, rest[:, half:])).astype(BF16)
    for t in range(4):
        out[:, 8 + t] = packed[:, t * LANES : (t + 1) * LANES].reshape(n_expert, ROWS, LANES)
    back.append(piece(out, back_hbm, 8, 4, back_sems.at[2]))
    back[2].start()
    for c in back:
        c.wait()


def mix_kernel(returned, sums, gate, place_first, place_low, place_high, mixed, importance, entropies):
    n_expert = returned.shape[0]
    wide = n_expert * ROWS
    width = mixed.shape[1]
    half = width // 2
    scale = gate[...]
    scale = jnp.concatenate([scale] * (half // LANES), axis=1)
    main = jnp.concatenate([returned[:, t].reshape(wide, LANES) for t in range(8)], axis=1)
    packed = jnp.concatenate([returned[:, 8 + t].reshape(wide, LANES) for t in range(4)], axis=1)
    chosen = mm(place_first[...], main[:, :half]) + mm(place_low[...], packed)
    mixed[:, :half] = (scale * chosen).astype(BF16)
    chosen = mm(place_first[...], main[:, half:]) + mm(place_high[...], packed)
    mixed[:, half:] = (scale * chosen).astype(BF16)
    total = sums[0:2]
    denom = jnp.maximum(total[:, n_expert : n_expert + 1], 1.0)
    mean = total[:, :n_expert] / denom
    importance[...] = mean
    terms = jnp.where(mean == 0.0, 0.0, mean * jnp.log(jnp.where(mean == 0.0, 1.0, mean)))
    spread = -jnp.sum(terms, axis=1, keepdims=True)
    token = total[:, n_expert + 1 : n_expert + 2] / denom
    entropies[...] = jnp.where(iota((2, 2), 1) == 0, token, spread)


def budget(kib):
    return pltpu.CompilerParams(vmem_limit_bytes=kib * 1024)


def out_of(shape, dtype):
    return jax.ShapeDtypeStruct(shape, dtype)


HBM = pl.BlockSpec(memory_space=pltpu.HBM)
VMEM = pl.BlockSpec(memory_space=pltpu.VMEM)


def per_device(tokens, router, w_in, w_out, assign, modality, slot):
    count, width = tokens.shape
    n_expert = router.shape[1]
    inner = w_in.shape[2]
    wide = n_expert * ROWS
    tiles = width // LANES * 3 // 2
    n_dp = lax.axis_size("dp")
    block = out_of((n_expert, tiles + 1, ROWS, LANES), BF16)
    ints = pltpu.VMEM((count,), I32)
    buffer, gate = pl.pallas_call(
        send_kernel,
        in_specs=[HBM] * 5,
        out_specs=(VMEM, VMEM),
        out_shape=(block, out_of((ROWS, count), F32)),
        scratch_shapes=[
            pltpu.VMEM((count, width), BF16),
            pltpu.VMEM((n_expert, width), BF16),
            ints,
            ints,
            ints,
            pltpu.SemaphoreType.DMA((5,)),
        ],
        name="send",
        compiler_params=budget(65472),
    )(tokens, router.T, assign, slot, modality)
    received = lax.all_to_all(buffer, "expert", split_axis=0, concat_axis=0, tiled=True)
    place = out_of((count, wide), BF16)
    scale, place_first, place_low, place_high, early = pl.pallas_call(
        place_kernel,
        in_specs=[VMEM] * 3 + [HBM],
        out_specs=(VMEM,) * 5,
        out_shape=(out_of((count, LANES), F32), place, place, place, out_of((width, EARLY), BF16)),
        scratch_shapes=[pltpu.SemaphoreType.DMA(())],
        name="place",
        compiler_params=budget(24576),
    )(gate, assign, slot, w_in)
    stats = pl.pallas_call(
        group_kernel,
        in_specs=[VMEM],
        out_specs=VMEM,
        out_shape=out_of((ROWS, LANES), F32),
        name="group",
        compiler_params=budget(24576),
    )(received)
    other = lax.ppermute(stats, "dp", [(d, d ^ 4) for d in range(n_dp)])
    matmuls = pl.pallas_call(
        ffn_kernel,
        in_specs=[VMEM, VMEM, HBM, HBM],
        out_specs=HBM,
        out_shape=out_of((n_expert, tiles, ROWS, LANES), BF16),
        scratch_shapes=[
            pltpu.VMEM((width, inner - EARLY), BF16),
            pltpu.VMEM((inner, width), BF16),
            pltpu.VMEM((wide * 3 // 2, width), BF16),
            pltpu.VMEM((wide * 3 // 2, inner), BF16),
            pltpu.VMEM((wide // 2, width), BF16),
            pltpu.VMEM((n_expert, tiles, ROWS, LANES), BF16),
            pltpu.SemaphoreType.DMA((8,)),
            pltpu.SemaphoreType.DMA((3,)),
        ],
        name="ffn",
        compiler_params=budget(50000),
    )
    computed = matmuls(received, early, w_in, w_out)
    returned = lax.all_to_all(computed, "expert", split_axis=0, concat_axis=0, tiled=True)
    near = [[4 * j + i for i in range(4)] for j in range(n_dp // 4)]
    far = [[8 * j + i for j in range(n_dp // 8)] for i in range(8)]
    stats = stats + other
    for groups in (near, far):
        stats = lax.psum(stats, "dp", axis_index_groups=groups)
    return pl.pallas_call(
        mix_kernel,
        in_specs=[VMEM] * 6,
        out_specs=(VMEM,) * 3,
        out_shape=(
            out_of((count, width), BF16),
            out_of((2, n_expert), F32),
            out_of((2, 2), F32),
        ),
        name="mix",
        compiler_params=budget(24576),
    )(returned, stats, scale, place_first, place_low, place_high)


def solution(mesh):
    placed = (
        P(BOTH, None),
        P(),
        P("expert", None, None),
        P("expert", None, None),
        P(BOTH),
        P(BOTH),
        P(BOTH),
    )
    return jax.shard_map(
        per_device,
        mesh=mesh,
        in_specs=placed,
        out_specs=(P(BOTH, None), P(), P()),
        check_vma=False,
    )
```
